512 devices in a mesh: modes: 16 (over y, core), gz: 32 (over x, z).
Axes of the slice: x: 4, y: 8, z: 8, core: 2. Of those that a mesh axis runs over, the one named last changes fastest.
Arguments:
- source_field: float32 [512, 2, 32, 2048], P('gz', None, None, 'modes'), may hold values from -0.075 to 0.075
- coupling_below: float32 [512], P('gz'), may hold values from 0.5 to 2
- coupling_above: float32 [512], P('gz'), may hold values from 0.5 to 2
- eigen_stream: float32 [32], replicated, may hold values from 0.000390625 to 0.015625
- eigen_span: float32 [2048], replicated, may hold values from 0.000390625 to 0.015625
Outputs:
- pressure: float32 [512, 2, 32, 2048], P('gz', None, 'modes')
The draws below stay inside these ranges and needn't reach their ends.
All inputs are finite; a program needn't handle non-finite values.
Results may differ from the reference program's by a relative error of at most 0.0003.
Values sent between devices are 32-bit elements; how exact they have to be, the bound alone decides.
A program may use at most 64 MiB of HBM per device.

```python
import math
import jax
import jax.numpy as jnp
from jax import lax

CZ = 16
KY = 2048
KX = 32
NZ = 512


def draw_source_field(key, part):
    spread = 0.2 / CZ
    dims = (NZ, 2, KX, KY)
    return jnp.clip(jax.random.normal(key, dims, jnp.float32), -6.0, 6.0) * spread


def shard_levels(own_key, shape, pieces, smallest, top_value):
    def one(axis_at, parts):
        heights = jax.random.uniform(jax.random.fold_in(jax.random.fold_in(own_key, 6), axis_at), (parts,), jnp.float32, smallest / len(pieces), top_value / len(pieces))
        return jnp.repeat(jnp.exp(heights), shape[axis_at] // parts).reshape((-1,) + (1,) * (len(shape) - axis_at - 1))

    factor_of = one(*pieces[0])
    for cut in pieces[1:]:
        factor_of = factor_of * one(*cut)
    return factor_of


def setup_inputs(seed: int = 0) -> dict:
    splits = jax.random.split(jax.random.key(seed), 6)
    return {
        "source_field": draw_source_field(jax.random.fold_in(splits[5], 71), 0),
        "coupling_below": jnp.clip(jnp.exp(math.log(2.0) - 1.3862944 * jax.random.uniform(splits[1], (NZ,), jnp.float32) ** shard_levels(splits[1], (NZ,), ((0, 32),), -0.2, 0.2)), 0.5, 2.0),
        "coupling_above": jnp.clip(jnp.exp(math.log(2.0) - 1.3862944 * jax.random.uniform(splits[2], (NZ,), jnp.float32) ** shard_levels(splits[2], (NZ,), ((0, 32),), -0.2, 0.2)), 0.5, 2.0),
        "eigen_stream": jnp.clip(jnp.exp(jax.random.uniform(splits[3], (KX,), jnp.float32, math.log(0.000390625), math.log(0.015625))), 0.000390625, 0.015625),
        "eigen_span": jnp.clip(jnp.exp(jax.random.uniform(splits[4], (KY,), jnp.float32, math.log(0.000390625), math.log(0.015625))), 0.000390625, 0.015625),
    }


def reference(source_field, coupling_below, coupling_above, eigen_stream, eigen_span):
    planes = jnp.arange(NZ)
    lower_coef = jnp.where(planes == 0, jnp.zeros_like(coupling_below), coupling_below)
    upper_coef = jnp.where(planes == NZ - 1, jnp.zeros_like(coupling_above), coupling_above)

    def per_stream(inputs):
        eigen_one, block = inputs
        spectral = eigen_one + eigen_span
        central = lower_coef[None, :] + upper_coef[None, :] + spectral[:, None]
        below_band = jnp.broadcast_to(-lower_coef[None, :], central.shape)
        above_band = jnp.broadcast_to(-upper_coef[None, :], central.shape)
        rights = jnp.transpose(block, (2, 0, 1))
        solved = lax.linalg.tridiagonal_solve(below_band, central, above_band, rights)
        return jnp.transpose(solved, (1, 2, 0))
    stacked = lax.map(per_stream, (eigen_stream, jnp.moveaxis(source_field, 2, 0)))
    return jnp.moveaxis(stacked, 0, 2)
```

```python
import functools

import jax
import jax.numpy as jnp
from jax import lax
from jax.experimental import pallas as pl
from jax.experimental.pallas import tpu as pltpu
from jax.sharding import PartitionSpec as P

MESH = pl.DeviceIdType.MESH
LANES = 128


def kernel(
    modes, parts,
    f_hbm, low_s, up_s, es_s, ep_ref,
    out_hbm,
    F, W, O, SAB, AB, CS, CR, GR, RS, XR, V, T, FAC, HQ, AL, GA, EI, LAM,
    load_sem, store_sem, y1_send, y1_recv, y2_send, y2_recv, c_send, c_recv, g_send, g_recv, r_send, r_recv,
):
    rows = F.shape[0]
    last = rows - 1
    step = parts // modes
    mi = lax.axis_index("modes")
    gi = lax.axis_index("gz")
    is_solver = lax.rem(gi, step) == 0
    my_block = gi // step

    load = pltpu.make_async_copy(f_hbm, F, load_sem)
    load.start()

    barrier = pltpu.get_barrier_semaphore()

    def signal_modes(r, _):
        pl.semaphore_signal(barrier, inc=1, device_id={"modes": lax.rem(mi + r, modes)}, device_id_type=MESH)
        return 0

    lax.fori_loop(1, modes, signal_modes, 0)

    @pl.when(is_solver)
    def _():
        def signal_all(r, _):
            pl.semaphore_signal(barrier, inc=1, device_id={"gz": lax.rem(gi + r, parts)}, device_id_type=MESH)
            return 0

        lax.fori_loop(1, parts, signal_all, 0)

    @pl.when(jnp.logical_not(is_solver))
    def _():
        def signal_solvers(j, _):
            pl.semaphore_signal(barrier, inc=1, device_id={"gz": j * step}, device_id_type=MESH)
            return 0

        lax.fori_loop(0, modes, signal_solvers, 0)

    low = [low_s[k] for k in range(rows)]
    up = [up_s[k] for k in range(rows)]
    low[0] = jnp.where(gi == 0, 0.0, low[0])
    up[last] = jnp.where(gi == parts - 1, 0.0, up[last])

    for b in range(2):
        LAM[:, pl.ds(b, 1), :] = (es_s[mi * 2 + b] + ep_ref[...]).reshape(modes, 1, LANES)
    lam = LAM[...]
    excess = lam + low[0]
    for k in range(last):
        inv = 1.0 / (up[k] + excess)
        factor = up[k] * inv
        if k == 0:
            qv = low[0] * inv
            qh = lam * inv
        else:
            qv = (low[k] * inv) * qv
            qh = (lam + low[k] * qh) * inv
        FAC[k] = factor
        V[k] = qv
        HQ[k] = qh
        excess = lam + low[k + 1] * (excess * inv)
    v, t, h = qv, factor, qh
    T[last - 1] = t
    CS[:, 0] = low[last] * v
    CS[:, 1] = lam + low[last] * h
    for k in range(last - 2, -1, -1):
        factor = FAC[k]
        v = V[k] + factor * v
        t = factor * t
        h = HQ[k] + factor * h
        V[k] = v
        T[k] = t
    CS[:, 2] = t
    CS[:, 3] = h
    CS[:, 4] = jnp.full_like(t, 1.0) * up[last]

    for j in range(modes):
        for b in range(2):
            LAM[j, pl.ds(b, 1), :] = es_s[2 * j + b] + ep_ref[pl.ds(mi, 1), :]
    lam = LAM[...]
    load.wait()
    excess = lam + low[0]
    q = [None, None]
    for k in range(last):
        inv = 1.0 / (up[k] + excess)
        FAC[k] = up[k] * inv
        for c in range(2):
            q[c] = (F[k, c] if k == 0 else F[k, c] + low[k] * q[c]) * inv
            F[k, c] = q[c]
        excess = lam + low[k + 1] * (excess * inv)
    for c in range(2):
        SAB[c] = F[last, c] + low[last] * q[c]
    for k in range(last - 2, -1, -1):
        factor = FAC[k]
        for c in range(2):
            q[c] = F[k, c] + factor * q[c]
            if k:
                F[k, c] = q[c]
            else:
                SAB[2 + c] = q[c]

    pl.semaphore_wait(barrier, jnp.where(is_solver, modes - 1 + parts - 1, modes - 1 + modes))

    def y1_copy(target, slot):
        return pltpu.make_async_remote_copy(
            src_ref=SAB.at[:, target], dst_ref=AB.at[:, slot],
            send_sem=y1_send.at[target], recv_sem=y1_recv.at[slot],
            device_id={"modes": target}, device_id_type=MESH)

    def y2_copy(target, slot):
        return pltpu.make_async_remote_copy(
            src_ref=F.at[pl.ds(1, last - 1), :, target], dst_ref=W.at[:, :, slot],
            send_sem=y2_send.at[target], recv_sem=y2_recv.at[slot],
            device_id={"modes": target}, device_id_type=MESH)

    def c_copy(block, slot):
        return pltpu.make_async_remote_copy(
            src_ref=CS.at[block], dst_ref=CR.at[slot],
            send_sem=c_send.at[block], recv_sem=c_recv.at[slot],
            device_id={"gz": block * step}, device_id_type=MESH)

    def g_copy(block, slot):
        return pltpu.make_async_remote_copy(
            src_ref=AB.at[:, block], dst_ref=GR.at[slot],
            send_sem=g_send.at[block], recv_sem=g_recv.at[slot],
            device_id={"gz": block * step}, device_id_type=MESH)

    def r_copy(part, slot):
        return pltpu.make_async_remote_copy(
            src_ref=RS.at[part], dst_ref=XR.at[slot],
            send_sem=r_send.at[part], recv_sem=r_recv.at[slot],
            device_id={"gz": part}, device_id_type=MESH)

    def spread(i):
        half = modes // 2
        return jnp.where(lax.rem(i, 2) == 0, half + i // 2, half - (i + 1) // 2)

    def start_y1(i, _):
        y1_copy(lax.rem(mi + spread(i), modes), mi).start()
        return 0

    def start_y2(i, _):
        y2_copy(lax.rem(mi + spread(i), modes), mi).start()
        return 0

    def start_c(j, _):
        @pl.when(j * step != gi)
        def _():
            c_copy(j, gi).start()

        return 0

    lax.fori_loop(0, modes - 1, start_y1, 0)
    lax.fori_loop(0, modes, start_c, 0)
    lax.fori_loop(0, modes - 1, start_y2, 0)

    AB[:, mi] = SAB[:, mi]
    W[:, :, mi] = F[1:last, :, mi]

    @pl.when(is_solver)
    def _():
        CR[gi] = CS[my_block]

    def forward(i, _):
        block = lax.rem(mi + i, modes)

        @pl.when(i > 0)
        def _():
            y1_copy(block, block).wait_recv()

        @pl.when(block * step != gi)
        def _():
            g_copy(block, gi).start()

        @pl.when(block * step == gi)
        def _():
            GR[gi] = AB[:, block]

        return 0

    lax.fori_loop(0, modes, forward, 0)

    def up_by(x, d, fill):
        return jnp.concatenate([x[d:], jnp.full((d,) + x.shape[1:], fill, x.dtype)], axis=0)

    def down_by(x, d, fill):
        return jnp.concatenate([jnp.full((d,) + x.shape[1:], fill, x.dtype), x[:-d]], axis=0)

    @pl.when(is_solver)
    def _():
        def wait_c(i, _):
            c_copy(my_block, lax.rem(gi + i, parts)).wait_recv()
            return 0

        lax.fori_loop(1, parts, wait_c, 0)
        a = CR[:, 0]
        u = CR[:, 4]
        c = u * up_by(CR[:, 2], 1, 0.0)
        e = CR[:, 1] + u * up_by(CR[:, 3], 1, 0.0)
        d, level = 1, 0
        while d < parts:
            inv = 1.0 / (a + c + e)
            alpha = a * down_by(inv, d, 0.0)
            gamma = c * up_by(inv, d, 0.0)
            AL[level] = alpha
            GA[level] = gamma
            e = e + alpha * down_by(e, d, 0.0) + gamma * up_by(e, d, 0.0)
            a = alpha * down_by(a, d, 0.0)
            c = gamma * up_by(c, d, 0.0)
            d, level = 2 * d, level + 1
        EI[...] = 1.0 / e

        def wait_g(i, _):
            g_copy(my_block, lax.rem(gi + i, parts)).wait_recv()
            return 0

        lax.fori_loop(1, parts, wait_g, 0)
        for p in range(2):
            x = GR[:, p] + u * up_by(GR[:, 2 + p], 1, 0.0)
            d, level = 1, 0
            while d < parts:
                x = x + AL[level] * down_by(x, d, 0.0) + GA[level] * up_by(x, d, 0.0)
                d, level = 2 * d, level + 1
            x = x * EI[...]
            RS[:, 1, p] = x
            RS[:, 0, p] = down_by(x, 1, 0.0)

        def start_r(i, _):
            r_copy(lax.rem(gi + i, parts), my_block).start()
            return 0

        lax.fori_loop(1, parts, start_r, 0)
        XR[my_block] = RS[gi]

    def wait_y2(i, _):
        slot = lax.rem(mi + i, modes)
        y2_copy(slot, slot).wait_recv()
        return 0

    lax.fori_loop(1, modes, wait_y2, 0)

    def wait_r(j, _):
        @pl.when(j * step != gi)
        def _():
            r_copy(gi, j).wait_recv()

        return 0

    lax.fori_loop(0, modes, wait_r, 0)

    for p in range(2):
        prev = XR[:, 0, p]
        own = XR[:, 1, p]
        O[last, p] = own
        O[0, p] = AB[2 + p] + V[0] * prev + T[0] * own
        for k in range(1, last):
            O[k, p] = W[k - 1, p] + V[k] * prev + T[k] * own

    def store(j):
        return pltpu.make_async_copy(
            O.at[:, :, j], out_hbm.at[:, :, :, pl.ds(pl.multiple_of(j * LANES, LANES), LANES)], store_sem.at[j])

    def start_store(j, _):
        store(j).start()
        return 0

    lax.fori_loop(0, modes, start_store, 0)

    def finish_modes(i, _):
        target = lax.rem(mi + i, modes)
        y1_copy(target, target).wait_send()
        y2_copy(target, target).wait_send()
        return 0

    lax.fori_loop(1, modes, finish_modes, 0)

    def finish_solvers(j, _):
        @pl.when(j * step != gi)
        def _():
            c_copy(j, gi).wait_send()
            g_copy(j, gi).wait_send()

        return 0

    lax.fori_loop(0, modes, finish_solvers, 0)

    @pl.when(is_solver)
    def _():
        def finish_r(i, _):
            part = lax.rem(gi + i, parts)
            r_copy(part, my_block).wait_send()
            return 0

        lax.fori_loop(1, parts, finish_r, 0)

    def finish_store(j, _):
        store(j).wait()
        return 0

    lax.fori_loop(0, modes, finish_store, 0)


def solution(mesh):
    modes, parts = mesh.shape["modes"], mesh.shape["gz"]

    def per_device(source_field, coupling_below, coupling_above, eigen_stream, eigen_span):
        rows, _, kx, _ = source_field.shape
        levels = (parts - 1).bit_length()
        f32 = jnp.float32
        tile = (2, LANES)
        vmem = lambda *shape: pltpu.VMEM(shape + tile, f32)
        dma = lambda *shape: pltpu.SemaphoreType.DMA(shape)
        return pl.pallas_call(
            functools.partial(kernel, modes, parts),
            out_shape=jax.ShapeDtypeStruct((rows, 2, kx // modes, modes * LANES), f32),
            in_specs=[
                pl.BlockSpec(memory_space=pl.ANY),
                pl.BlockSpec(memory_space=pltpu.SMEM),
                pl.BlockSpec(memory_space=pltpu.SMEM),
                pl.BlockSpec(memory_space=pltpu.SMEM),
                pl.BlockSpec(memory_space=pltpu.VMEM),
            ],
            out_specs=pl.BlockSpec(memory_space=pl.ANY),
            scratch_shapes=[
                vmem(rows, 2, modes), vmem(rows - 2, 2, modes), vmem(rows, 2, modes),
                vmem(4, modes), vmem(4, modes),
                vmem(modes, 5), vmem(parts, 5), vmem(parts, 4), vmem(parts, 2, 2), vmem(modes, 2, 2),
                vmem(rows - 1, modes), vmem(rows - 1, modes), vmem(rows - 1, modes), vmem(rows - 1, modes),
                vmem(levels, parts), vmem(levels, parts), vmem(parts), vmem(modes),
                dma(), dma(modes), dma(modes), dma(modes), dma(modes), dma(modes),
                dma(modes), dma(parts), dma(modes), dma(parts), dma(parts), dma(modes),
            ],
            compiler_params=pltpu.CompilerParams(collective_id=0, has_side_effects=True),
        )(
            source_field.reshape(rows, 2, modes, 2, LANES),
            coupling_below, coupling_above, eigen_stream, eigen_span.reshape(modes, LANES),
        )

    return jax.shard_map(
        per_device,
        mesh=mesh,
        in_specs=(P("gz", None, None, "modes"), P("gz"), P("gz"), P(), P()),
        out_specs=P("gz", None, "modes", None),
        check_vma=False,
    )
```

```python
import functools

import jax
import jax.numpy as jnp
from jax import lax
from jax.experimental import pallas as pl
from jax.experimental.pallas import tpu as pltpu
from jax.sharding import PartitionSpec as P

MESH = pl.DeviceIdType.MESH
LANES = 128


def gz_columns(parts):
    return min(4, parts // 2)


def spread(i, half):
    return jnp.where(lax.rem(i, 2) == 0, half + i // 2, half - (i + 1) // 2)


def exchange_kernel(
    modes, parts,
    f_hbm, low_hbm, up_hbm, es_hbm, ep_hbm,
    W, XR, V, T,
    F, SAB, CS, CR, GR, RS, FAC, HQ, AL, GA, EI, LAM, EP, low_s, up_s, es_s,
    load_sem, y_send, y_recv, ab_send, ab_recv, c_send, c_recv, r_send, r_recv,
):
    rows = F.shape[0]
    last = rows - 1
    half = modes // 4
    cols = gz_columns(parts)
    depth = parts // cols
    mi = lax.axis_index("modes")
    gi = lax.axis_index("gz")

    def home(j):
        d = j // 2 - half
        r = jnp.where(d > 0, 2 * d, jnp.where(d < 0, -2 * d - 1, 0)) * 2 + lax.rem(j, 2)
        return lax.rem(r, cols) * depth + r // cols

    rank = lax.rem(gi, depth) * cols + gi // depth
    is_solver = rank < modes
    my_block = spread(jnp.minimum(rank, modes - 1) // 2, half) * 2 + lax.rem(rank, 2)
    my_home = home(mi)

    loads = [
        pltpu.make_async_copy(src, dst, load_sem.at[i])
        for i, (src, dst) in enumerate(
            [(f_hbm, F), (low_hbm, low_s), (up_hbm, up_s), (es_hbm, es_s), (ep_hbm, EP)])
    ]
    for copy in loads:
        copy.start()

    barrier = pltpu.get_barrier_semaphore()

    def signal_modes(r, _):
        pl.semaphore_signal(barrier, inc=1, device_id={"modes": lax.rem(mi + r, modes)}, device_id_type=MESH)
        return 0

    lax.fori_loop(1, modes, signal_modes, 0)

    @pl.when(is_solver)
    def _():
        def signal_parts(r, _):
            part = lax.rem(gi + r, parts)
            pl.semaphore_signal(barrier, inc=1, device_id={"gz": part}, device_id_type=MESH)
            pl.semaphore_signal(barrier, inc=1, device_id={"modes": my_block, "gz": part}, device_id_type=MESH)
            return 0

        lax.fori_loop(1, parts, signal_parts, 0)

        @pl.when(my_block != mi)
        def _():
            pl.semaphore_signal(barrier, inc=1, device_id={"modes": my_block}, device_id_type=MESH)

    for copy in loads[1:]:
        copy.wait()
    low = [low_s[k] for k in range(rows)]
    up = [up_s[k] for k in range(rows)]
    low[0] = jnp.where(gi == 0, 0.0, low[0])
    up[last] = jnp.where(gi == parts - 1, 0.0, up[last])

    for j in range(modes):
        for b in range(2):
            LAM[j, pl.ds(b, 1), :] = es_s[2 * j + b] + EP[pl.ds(mi, 1), :]
    lam = LAM[...]
    loads[0].wait()
    excess = lam + low[0]
    q = [None, None]
    for k in range(last):
        inv = 1.0 / (up[k] + excess)
        FAC[k] = up[k] * inv
        for c in range(2):
            q[c] = (F[k, c] if k == 0 else F[k, c] + low[k] * q[c]) * inv
            F[k, c] = q[c]
        excess = lam + low[k + 1] * (excess * inv)
    for c in range(2):
        SAB[c] = F[last, c] + low[last] * q[c]
    for k in range(last - 2, -1, -1):
        factor = FAC[k]
        for c in range(2):
            q[c] = F[k, c] + factor * q[c]
            F[k, c] = q[c]
    for c in range(2):
        SAB[2 + c] = q[c]

    def ab_copy(target, slot):
        return pltpu.make_async_remote_copy(
            src_ref=SAB.at[:, target], dst_ref=GR.at[slot],
            send_sem=ab_send.at[target], recv_sem=ab_recv.at[slot],
            device_id={"modes": target, "gz": my_home}, device_id_type=MESH)

    def y_copy(target, slot):
        return pltpu.make_async_remote_copy(
            src_ref=F.at[pl.ds(0, last), :, target], dst_ref=W.at[:, :, slot],
            send_sem=y_send.at[target], recv_sem=y_recv.at[slot],
            device_id={"modes": target}, device_id_type=MESH)

    def c_copy(block, slot):
        return pltpu.make_async_remote_copy(
            src_ref=CS.at[block], dst_ref=CR.at[slot],
            send_sem=c_send.at[block], recv_sem=c_recv.at[slot],
            device_id={"gz": home(block)}, device_id_type=MESH)

    def r_copy(part, slot):
        return pltpu.make_async_remote_copy(
            src_ref=RS.at[part], dst_ref=XR.at[slot],
            send_sem=r_send.at[part], recv_sem=r_recv.at[slot],
            device_id={"gz": part}, device_id_type=MESH)

    solver_i = jnp.where(is_solver, 1, 0)
    home_i = jnp.where(my_home == gi, 1, 0)
    pl.semaphore_wait(barrier, (modes - 1) + (modes - home_i) + (modes - solver_i))

    def start_ab(i, _):
        target = lax.rem(mi + spread(i, modes // 2), modes)

        @pl.when(jnp.logical_or(target != mi, my_home != gi))
        def _():
            ab_copy(target, gi).start()

        return 0

    lax.fori_loop(0, modes, start_ab, 0)

    def start_y(i, _):
        y_copy(lax.rem(mi + spread(i, modes // 2), modes), mi).start()
        return 0

    lax.fori_loop(0, modes - 1, start_y, 0)
    W[:, :, mi] = F[0:last, :, mi]

    @pl.when(my_home == gi)
    def _():
        GR[gi] = SAB[:, mi]

    for b in range(2):
        LAM[:, pl.ds(b, 1), :] = (es_s[mi * 2 + b] + EP[...]).reshape(modes, 1, LANES)
    lam = LAM[...]
    excess = lam + low[0]
    for k in range(last):
        inv = 1.0 / (up[k] + excess)
        factor = up[k] * inv
        if k == 0:
            qv = low[0] * inv
            qh = lam * inv
        else:
            qv = (low[k] * inv) * qv
            qh = (lam + low[k] * qh) * inv
        FAC[k] = factor
        V[k] = qv
        HQ[k] = qh
        excess = lam + low[k + 1] * (excess * inv)
    v, t, h = qv, factor, qh
    T[last - 1] = t
    CS[:, 0] = low[last] * v
    CS[:, 1] = lam + low[last] * h
    for k in range(last - 2, -1, -1):
        factor = FAC[k]
        v = V[k] + factor * v
        t = factor * t
        h = HQ[k] + factor * h
        V[k] = v
        T[k] = t
    CS[:, 2] = t
    CS[:, 3] = h
    CS[:, 4] = jnp.full_like(t, 1.0) * up[last]

    def start_c(j, _):
        @pl.when(home(j) != gi)
        def _():
            c_copy(j, gi).start()

        return 0

    lax.fori_loop(0, modes, start_c, 0)

    def up_by(x, d, fill):
        return jnp.concatenate([x[d:], jnp.full((d,) + x.shape[1:], fill, x.dtype)], axis=0)

    def down_by(x, d, fill):
        return jnp.concatenate([jnp.full((d,) + x.shape[1:], fill, x.dtype), x[:-d]], axis=0)

    @pl.when(is_solver)
    def _():
        CR[gi] = CS[my_block]

        def wait_c(i, _):
            c_copy(my_block, lax.rem(gi + i, parts)).wait_recv()
            return 0

        lax.fori_loop(1, parts, wait_c, 0)
        a = CR[:, 0]
        u = CR[:, 4]
        c = u * up_by(CR[:, 2], 1, 0.0)
        e = CR[:, 1] + u * up_by(CR[:, 3], 1, 0.0)
        d, level = 1, 0
        while d < parts:
            inv = 1.0 / (a + c + e)
            alpha = a * down_by(inv, d, 0.0)
            gamma = c * up_by(inv, d, 0.0)
            AL[level] = alpha
            GA[level] = gamma
            e = e + alpha * down_by(e, d, 0.0) + gamma * up_by(e, d, 0.0)
            a = alpha * down_by(a, d, 0.0)
            c = gamma * up_by(c, d, 0.0)
            d, level = 2 * d, level + 1
        EI[...] = 1.0 / e

        def wait_ab(part, _):
            @pl.when(jnp.logical_or(my_block != mi, part != gi))
            def _():
                ab_copy(mi, part).wait_recv()

            return 0

        lax.fori_loop(0, parts, wait_ab, 0)
        for p in range(2):
            x = GR[:, p] + u * up_by(GR[:, 2 + p], 1, 0.0)
            d, level = 1, 0
            while d < parts:
                x = x + AL[level] * down_by(x, d, 0.0) + GA[level] * up_by(x, d, 0.0)
                d, level = 2 * d, level + 1
            x = x * EI[...]
            RS[:, 1, p] = x
            RS[:, 0, p] = down_by(x, 1, 0.0)

        def start_r(i, _):
            part = lax.rem(i, cols) * depth + i // cols

            @pl.when(part != gi)
            def _():
                r_copy(part, my_block).start()

            return 0

        lax.fori_loop(0, parts, start_r, 0)
        XR[my_block] = RS[gi]

    def wait_y(i, _):
        slot = lax.rem(mi + i, modes)
        y_copy(slot, slot).wait_recv()
        return 0

    lax.fori_loop(1, modes, wait_y, 0)

    def finish_modes(i, _):
        target = lax.rem(mi + i, modes)
        y_copy(target, target).wait_send()
        return 0

    lax.fori_loop(1, modes, finish_modes, 0)

    def finish_solvers(j, _):
        @pl.when(jnp.logical_or(j != mi, my_home != gi))
        def _():
            ab_copy(j, gi).wait_send()

        @pl.when(home(j) != gi)
        def _():
            c_copy(j, gi).wait_send()

        return 0

    lax.fori_loop(0, modes, finish_solvers, 0)

    @pl.when(is_solver)
    def _():
        def finish_r(i, _):
            r_copy(lax.rem(gi + i, parts), my_block).wait_send()
            return 0

        lax.fori_loop(1, parts, finish_r, 0)

    def wait_r(j, _):
        @pl.when(home(j) != gi)
        def _():
            r_copy(gi, j).wait_recv()

        return 0

    lax.fori_loop(0, modes, wait_r, 0)


def combine_kernel(W, XR, V, T, out_hbm, O, store_sem):
    rows, modes = O.shape[0], V.shape[1]
    last = rows - 1
    stores = [pltpu.make_async_copy(O.at[k], out_hbm.at[k], store_sem.at[k]) for k in range(rows)]
    for k in range(rows):
        for p in range(2):
            own = XR[:, 1, p]
            value = own if k == last else W[k, p] + V[k] * XR[:, 0, p] + T[k] * own
            for j in range(modes):
                O[k, p, :, pl.ds(j * LANES, LANES)] = value[j]
        stores[k].start()
    for copy in stores:
        copy.wait()


def solution(mesh):
    modes, parts = mesh.shape["modes"], mesh.shape["gz"]

    def per_device(source_field, coupling_below, coupling_above, eigen_stream, eigen_span):
        rows, _, kx, _ = source_field.shape
        levels = (parts - 1).bit_length()
        f32 = jnp.float32
        tile = (2, LANES)
        vmem = lambda *shape: pltpu.VMEM(shape + tile, f32)
        dma = lambda *shape: pltpu.SemaphoreType.DMA(shape)
        smem = lambda n: pltpu.SMEM((n,), f32)
        anywhere = pl.BlockSpec(memory_space=pl.ANY)
        local = pl.BlockSpec(memory_space=pltpu.VMEM)
        arrived = pl.pallas_call(
            functools.partial(exchange_kernel, modes, parts),
            out_shape=[
                vmem(rows - 1, 2, modes), vmem(modes, 2, 2), vmem(rows - 1, modes), vmem(rows - 1, modes),
            ],
            in_specs=[anywhere] * 5,
            out_specs=[local] * 4,
            scratch_shapes=[
                vmem(rows, 2, modes),
                vmem(4, modes), vmem(modes, 5), vmem(parts, 5), vmem(parts, 4), vmem(parts, 2, 2),
                vmem(rows - 1, modes), vmem(rows - 1, modes),
                vmem(levels, parts), vmem(levels, parts), vmem(parts), vmem(modes),
                pltpu.VMEM((modes, LANES), f32), smem(rows), smem(rows), smem(kx),
                dma(5), dma(modes), dma(modes), dma(modes), dma(parts), dma(modes), dma(parts), dma(parts), dma(modes),
            ],
            compiler_params=pltpu.CompilerParams(collective_id=0, has_side_effects=True),
        )(
            source_field.reshape(rows, 2, modes, 2, LANES),
            coupling_below, coupling_above, eigen_stream, eigen_span.reshape(modes, LANES),
        )
        return pl.pallas_call(
            combine_kernel,
            out_shape=jax.ShapeDtypeStruct((rows, 2, kx // modes, modes * LANES), f32),
            in_specs=[local] * 4,
            out_specs=anywhere,
            scratch_shapes=[pltpu.VMEM((rows, 2, kx // modes, modes * LANES), f32), dma(rows)],
            compiler_params=pltpu.CompilerParams(vmem_limit_bytes=4 << 20),
        )(*[pltpu.with_memory_space_constraint(x, pltpu.VMEM) for x in arrived])

    return jax.shard_map(
        per_device,
        mesh=mesh,
        in_specs=(P("gz", None, None, "modes"), P("gz"), P("gz"), P(), P()),
        out_specs=P("gz", None, "modes", None),
        check_vma=False,
    )
```

```python
import functools

import jax
import jax.numpy as jnp
from jax import lax
from jax.experimental import pallas as pl
from jax.experimental.pallas import tpu as pltpu
from jax.sharding import PartitionSpec as P

MESH = pl.DeviceIdType.MESH
LANES = 128


def gz_columns(parts):
    return min(4, parts // 2)


def spread(i, half):
    return jnp.where(lax.rem(i, 2) == 0, half + i // 2, half - (i + 1) // 2)


def exchange_kernel(
    modes, parts,
    f_hbm, low_hbm, up_hbm, es_hbm, ep_hbm,
    W, XR, V, T,
    F, SAB, AB, CS, CR, GR, RS, FAC, AL, GA, EI, PK, LAM, EP, low_s, up_s, es_s,
    load_sem, y_send, y_recv, s_send, s_recv, ab_send, ab_recv, c_send, c_recv, r_send, r_recv,
):
    rows = F.shape[0]
    last = rows - 1
    half = modes // 4
    cols = gz_columns(parts)
    depth = parts // cols
    mi = lax.axis_index("modes")
    gi = lax.axis_index("gz")

    def home(j):
        d = j // 2 - half
        r = jnp.where(d > 0, 2 * d, jnp.where(d < 0, -2 * d - 1, 0)) * 2 + lax.rem(j, 2)
        return lax.rem(r, cols) * depth + r // cols

    rank = lax.rem(gi, depth) * cols + gi // depth
    is_solver = rank < modes
    my_block = spread(jnp.minimum(rank, modes - 1) // 2, half) * 2 + lax.rem(rank, 2)
    my_home = home(mi)
    is_late = lax.rem(gi, depth) >= depth // 2

    loads = [
        pltpu.make_async_copy(src, dst, load_sem.at[i])
        for i, (src, dst) in enumerate(
            [(f_hbm, F), (low_hbm, low_s), (up_hbm, up_s), (es_hbm, es_s), (ep_hbm, EP)])
    ]
    for copy in loads:
        copy.start()

    barrier = pltpu.get_barrier_semaphore()

    def signal_modes(r, _):
        pl.semaphore_signal(barrier, inc=1, device_id={"modes": lax.rem(mi + r, modes)}, device_id_type=MESH)
        return 0

    lax.fori_loop(1, modes, signal_modes, 0)

    @pl.when(is_solver)
    def _():
        def signal_parts(r, _):
            part = lax.rem(gi + r, parts)
            pl.semaphore_signal(barrier, inc=1, device_id={"gz": part}, device_id_type=MESH)

            @pl.when(lax.rem(part, depth) >= depth // 2)
            def _():
                pl.semaphore_signal(barrier, inc=1, device_id={"modes": my_block, "gz": part}, device_id_type=MESH)

            return 0

        lax.fori_loop(1, parts, signal_parts, 0)

    for copy in loads[1:]:
        copy.wait()
    low = [low_s[k] for k in range(rows)]
    up = [up_s[k] for k in range(rows)]
    low[0] = jnp.where(gi == 0, 0.0, low[0])
    up[last] = jnp.where(gi == parts - 1, 0.0, up[last])

    lane = lax.broadcasted_iota(jnp.int32, (2, LANES), 1)
    packed = jnp.zeros((2, LANES), jnp.float32)
    for k in range(rows):
        packed = jnp.where(lane == k, low[k], packed)
        packed = jnp.where(lane == rows + k, up[k], packed)
    CS[...] = packed

    for j in range(modes):
        for b in range(2):
            LAM[j, pl.ds(b, 1), :] = es_s[2 * j + b] + EP[pl.ds(mi, 1), :]
    lam = LAM[...]
    loads[0].wait()
    excess = lam + low[0]
    q = [None, None]
    for k in range(last):
        inv = 1.0 / (up[k] + excess)
        FAC[k] = up[k] * inv
        for c in range(2):
            q[c] = (F[k, c] if k == 0 else F[k, c] + low[k] * q[c]) * inv
            F[k, c] = q[c]
        excess = lam + low[k + 1] * (excess * inv)
    for c in range(2):
        SAB[c] = F[last, c] + low[last] * q[c]
    for k in range(last - 2, -1, -1):
        factor = FAC[k]
        for c in range(2):
            q[c] = F[k, c] + factor * q[c]
            F[k, c] = q[c]
    for c in range(2):
        SAB[2 + c] = q[c]

    def s_copy(target, slot):
        return pltpu.make_async_remote_copy(
            src_ref=SAB.at[:, target], dst_ref=AB.at[:, slot],
            send_sem=s_send.at[target], recv_sem=s_recv.at[slot],
            device_id={"modes": target}, device_id_type=MESH)

    def forward_copy(block, slot):
        return pltpu.make_async_remote_copy(
            src_ref=AB.at[:, block], dst_ref=GR.at[slot],
            send_sem=ab_send.at[block], recv_sem=ab_recv.at[slot],
            device_id={"gz": home(block)}, device_id_type=MESH)

    def direct_copy(target, slot):
        return pltpu.make_async_remote_copy(
            src_ref=SAB.at[:, target], dst_ref=GR.at[slot],
            send_sem=ab_send.at[target], recv_sem=ab_recv.at[slot],
            device_id={"modes": target, "gz": my_home}, device_id_type=MESH)

    def y_copy(target, slot):
        return pltpu.make_async_remote_copy(
            src_ref=F.at[pl.ds(0, last), :, target], dst_ref=W.at[:, :, slot],
            send_sem=y_send.at[target], recv_sem=y_recv.at[slot],
            device_id={"modes": target}, device_id_type=MESH)

    def c_copy(block, slot):
        return pltpu.make_async_remote_copy(
            src_ref=CS, dst_ref=CR.at[slot],
            send_sem=c_send.at[block], recv_sem=c_recv.at[slot],
            device_id={"gz": home(block)}, device_id_type=MESH)

    def r_copy(part, slot):
        return pltpu.make_async_remote_copy(
            src_ref=RS.at[part], dst_ref=XR.at[slot],
            send_sem=r_send.at[part], recv_sem=r_recv.at[slot],
            device_id={"gz": part}, device_id_type=MESH)

    solver_i = jnp.where(is_solver, 1, 0)
    late_i = jnp.where(is_late, modes, 0)
    pl.semaphore_wait(barrier, (modes - 1) + (modes - solver_i) + late_i)

    @pl.when(is_late)
    def _():
        def start_direct(i, _):
            direct_copy(lax.rem(mi + spread(i, modes // 2), modes), gi).start()
            return 0

        lax.fori_loop(0, modes, start_direct, 0)

    @pl.when(jnp.logical_not(is_late))
    def _():
        def start_s(i, _):
            s_copy(lax.rem(mi + spread(i, modes // 2), modes), mi).start()
            return 0

        lax.fori_loop(0, modes - 1, start_s, 0)
        AB[:, mi] = SAB[:, mi]

    def start_c(j, _):
        @pl.when(home(j) != gi)
        def _():
            c_copy(j, gi).start()

        return 0

    lax.fori_loop(0, modes, start_c, 0)

    def start_y(i, _):
        y_copy(lax.rem(mi + spread(i, modes // 2), modes), mi).start()
        return 0

    lax.fori_loop(0, modes - 1, start_y, 0)
    W[:, :, mi] = F[0:last, :, mi]

    for b in range(2):
        LAM[:, pl.ds(b, 1), :] = (es_s[mi * 2 + b] + EP[...]).reshape(modes, 1, LANES)
    lam = LAM[...]
    excess = lam + low[0]
    for k in range(last):
        inv = 1.0 / (up[k] + excess)
        factor = up[k] * inv
        v = low[0] * inv if k == 0 else (low[k] * inv) * v
        FAC[k] = factor
        V[k] = v
        excess = lam + low[k + 1] * (excess * inv)
    t = factor
    T[last - 1] = t
    for k in range(last - 2, -1, -1):
        factor = FAC[k]
        v = V[k] + factor * v
        t = factor * t
        V[k] = v
        T[k] = t

    @pl.when(jnp.logical_not(is_late))
    def _():
        def forward(i, _):
            block = lax.rem(mi + i, modes)

            @pl.when(i > 0)
            def _():
                s_copy(block, block).wait_recv()

            @pl.when(home(block) != gi)
            def _():
                forward_copy(block, gi).start()

            @pl.when(home(block) == gi)
            def _():
                GR[gi] = AB[:, block]

            return 0

        lax.fori_loop(0, modes, forward, 0)

    count = 2 * parts

    def ahead(x, d):
        return pltpu.roll(x, count - 2 * d, 0)

    def behind(x, d):
        return pltpu.roll(x, 2 * d, 0)

    def spread_lane(x, k):
        return jnp.broadcast_to(x[:, k:k + 1], (count, LANES))

    @pl.when(is_solver)
    def _():
        CR[gi] = CS[...]

        def wait_c(i, _):
            c_copy(my_block, lax.rem(gi + i, parts)).wait_recv()
            return 0

        lax.fori_loop(1, parts, wait_c, 0)
        PK[0] = CR[...].reshape(count, LANES)
        couplings = PK[0]
        odd = lax.rem(lax.broadcasted_iota(jnp.int32, (count, LANES), 0), 2) == 1
        stream = jnp.where(odd, es_s[mi * 2 + 1], es_s[mi * 2])
        lam = stream + jnp.broadcast_to(EP[pl.ds(my_block, 1), :], (count, LANES))
        for k in range(last):
            lo = spread_lane(couplings, k)
            hi = spread_lane(couplings, rows + k)
            excess = lam + lo if k == 0 else lam + lo * (excess * inv)
            inv = 1.0 / (hi + excess)
            factor = hi * inv
            if k == 0:
                v = lo * inv
                qh = lam * inv
                h = qh
                t = factor
            else:
                v = (lo * inv) * v
                qh = (lam + lo * qh) * inv
                h = h + t * qh
                t = t * factor
        lo = spread_lane(couplings, last)
        u = spread_lane(couplings, rows + last)
        a = lo * v
        c = u * ahead(t, 1)
        e = lam + lo * qh + u * ahead(h, 1)
        d, level = 1, 0
        while d < parts:
            inv = 1.0 / (a + c + e)
            alpha = a * behind(inv, d)
            gamma = c * ahead(inv, d)
            AL[level] = alpha
            GA[level] = gamma
            e = e + alpha * behind(e, d) + gamma * ahead(e, d)
            a = alpha * behind(a, d)
            c = gamma * ahead(c, d)
            d, level = 2 * d, level + 1
        EI[...] = 1.0 / e

        def wait_ab(part, _):
            @pl.when(part != gi)
            def _():
                direct_copy(mi, part).wait_recv()

            return 0

        lax.fori_loop(0, parts, wait_ab, 0)
        for p in range(2):
            PK[0] = GR[:, p].reshape(count, LANES)
            PK[1] = GR[:, 2 + p].reshape(count, LANES)
            x = PK[0] + u * ahead(PK[1], 1)
            d, level = 1, 0
            while d < parts:
                x = x + AL[level] * behind(x, d) + GA[level] * ahead(x, d)
                d, level = 2 * d, level + 1
            x = x * EI[...]
            RS[:, 1, p] = x.reshape(parts, 2, LANES)
            RS[:, 0, p] = behind(x, 1).reshape(parts, 2, LANES)

        def start_r(i, _):
            part = lax.rem(i, cols) * depth + i // cols

            @pl.when(part != gi)
            def _():
                r_copy(part, my_block).start()

            return 0

        lax.fori_loop(0, parts, start_r, 0)
        XR[my_block] = RS[gi]

    def wait_y(i, _):
        slot = lax.rem(mi + i, modes)
        y_copy(slot, slot).wait_recv()
        return 0

    lax.fori_loop(1, modes, wait_y, 0)

    def finish_modes(i, _):
        target = lax.rem(mi + i, modes)
        y_copy(target, target).wait_send()
        return 0

    lax.fori_loop(1, modes, finish_modes, 0)

    def finish_solvers(j, _):
        @pl.when(home(j) != gi)
        def _():
            c_copy(j, gi).wait_send()
            forward_copy(j, gi).wait_send()

        return 0

    lax.fori_loop(0, modes, finish_solvers, 0)

    @pl.when(jnp.logical_not(is_late))
    def _():
        def finish_s(i, _):
            target = lax.rem(mi + i, modes)
            s_copy(target, target).wait_send()
            return 0

        lax.fori_loop(1, modes, finish_s, 0)

    @pl.when(is_solver)
    def _():
        def finish_r(i, _):
            r_copy(lax.rem(gi + i, parts), my_block).wait_send()
            return 0

        lax.fori_loop(1, parts, finish_r, 0)

    def wait_r(j, _):
        @pl.when(home(j) != gi)
        def _():
            r_copy(gi, j).wait_recv()

        return 0

    lax.fori_loop(0, modes, wait_r, 0)


def combine_kernel(W, XR, V, T, out_hbm, O, store_sem):
    rows, modes = O.shape[0], V.shape[1]
    last = rows - 1
    stores = [pltpu.make_async_copy(O.at[k], out_hbm.at[k], store_sem.at[k]) for k in range(rows)]
    for k in range(rows):
        for p in range(2):
            own = XR[:, 1, p]
            value = own if k == last else W[k, p] + V[k] * XR[:, 0, p] + T[k] * own
            for j in range(modes):
                O[k, p, :, pl.ds(j * LANES, LANES)] = value[j]
        stores[k].start()
    for copy in stores:
        copy.wait()


def solution(mesh):
    modes, parts = mesh.shape["modes"], mesh.shape["gz"]

    def per_device(source_field, coupling_below, coupling_above, eigen_stream, eigen_span):
        rows, _, kx, _ = source_field.shape
        levels = (parts - 1).bit_length()
        f32 = jnp.float32
        tile = (2, LANES)
        vmem = lambda *shape: pltpu.VMEM(shape + tile, f32)
        flat = lambda *shape: pltpu.VMEM(shape + (2 * parts, LANES), f32)
        dma = lambda *shape: pltpu.SemaphoreType.DMA(shape)
        smem = lambda n: pltpu.SMEM((n,), f32)
        anywhere = pl.BlockSpec(memory_space=pl.ANY)
        local = pl.BlockSpec(memory_space=pltpu.VMEM)
        arrived = pl.pallas_call(
            functools.partial(exchange_kernel, modes, parts),
            out_shape=[
                vmem(rows - 1, 2, modes), vmem(modes, 2, 2), vmem(rows - 1, modes), vmem(rows - 1, modes),
            ],
            in_specs=[anywhere] * 5,
            out_specs=[local] * 4,
            scratch_shapes=[
                vmem(rows, 2, modes),
                vmem(4, modes), vmem(4, modes), vmem(), vmem(parts), vmem(parts, 4), vmem(parts, 2, 2),
                vmem(rows - 1, modes),
                flat(levels), flat(levels), flat(), flat(2), vmem(modes),
                pltpu.VMEM((modes, LANES), f32), smem(rows), smem(rows), smem(kx),
                dma(5), dma(modes), dma(modes), dma(modes), dma(modes),
                dma(modes), dma(parts), dma(modes), dma(parts), dma(parts), dma(modes),
            ],
            compiler_params=pltpu.CompilerParams(collective_id=0, has_side_effects=True),
        )(
            source_field.reshape(rows, 2, modes, 2, LANES),
            coupling_below, coupling_above, eigen_stream, eigen_span.reshape(modes, LANES),
        )
        return pl.pallas_call(
            combine_kernel,
            out_shape=jax.ShapeDtypeStruct((rows, 2, kx // modes, modes * LANES), f32),
            in_specs=[local] * 4,
            out_specs=anywhere,
            scratch_shapes=[pltpu.VMEM((rows, 2, kx // modes, modes * LANES), f32), dma(rows)],
            compiler_params=pltpu.CompilerParams(vmem_limit_bytes=4 << 20),
        )(*[pltpu.with_memory_space_constraint(x, pltpu.VMEM) for x in arrived])

    return jax.shard_map(
        per_device,
        mesh=mesh,
        in_specs=(P("gz", None, None, "modes"), P("gz"), P("gz"), P(), P()),
        out_specs=P("gz", None, "modes", None),
        check_vma=False,
    )
```

```python
import functools

import jax
import jax.numpy as jnp
from jax import lax
from jax.experimental import pallas as pl
from jax.experimental.pallas import tpu as pltpu
from jax.sharding import PartitionSpec as P

MESH = pl.DeviceIdType.MESH
LANES = 128


def gz_columns(parts):
    return min(4, parts // 2)


def spread(i, half):
    return jnp.where(lax.rem(i, 2) == 0, half + i // 2, half - (i + 1) // 2)


def exchange_kernel(
    modes, parts,
    f_hbm, low_hbm, up_hbm, es_hbm, ep_hbm,
    W, XR, V, T,
    F, SAB, AB, CS, CR, GR, RS, FAC, AL, GA, EI, PK, LAM, EP, low_s, up_s, es_s,
    load_sem, y_send, y_recv, s_send, s_recv, ab_send, ab_recv, c_send, c_recv, r_send, r_recv,
):
    rows = F.shape[0]
    last = rows - 1
    half = modes // 4
    cols = gz_columns(parts)
    depth = parts // cols
    mi = lax.axis_index("modes")
    gi = lax.axis_index("gz")

    moved = (modes - 2, 4) if (modes, parts) == (16, 32) else None

    def home(j):
        d = j // 2 - half
        r = jnp.where(d > 0, 2 * d, jnp.where(d < 0, -2 * d - 1, 0)) * 2 + lax.rem(j, 2)
        site = lax.rem(r, cols) * depth + r // cols
        return jnp.where(r == moved[0], moved[1], site) if moved else site

    rank = lax.rem(gi, depth) * cols + gi // depth
    if moved:
        rank = jnp.where(gi == moved[1], moved[0], jnp.where(rank == moved[0], modes, rank))
    is_solver = rank < modes
    my_block = spread(jnp.minimum(rank, modes - 1) // 2, half) * 2 + lax.rem(rank, 2)
    my_home = home(mi)
    def late(part):
        z_late = lax.rem(part, depth) >= depth // 2
        return jnp.logical_and(z_late, part != moved[1]) if moved else z_late

    is_late = late(gi)

    loads = [
        pltpu.make_async_copy(src, dst, load_sem.at[i])
        for i, (src, dst) in enumerate(
            [(f_hbm, F), (low_hbm, low_s), (up_hbm, up_s), (es_hbm, es_s), (ep_hbm, EP)])
    ]
    for copy in loads:
        copy.start()

    barrier = pltpu.get_barrier_semaphore()

    def signal_modes(r, _):
        pl.semaphore_signal(barrier, inc=1, device_id={"modes": lax.rem(mi + r, modes)}, device_id_type=MESH)
        return 0

    lax.fori_loop(1, modes, signal_modes, 0)

    @pl.when(is_solver)
    def _():
        def signal_parts(r, _):
            part = lax.rem(gi + r, parts)
            pl.semaphore_signal(barrier, inc=1, device_id={"gz": part}, device_id_type=MESH)

            @pl.when(late(part))
            def _():
                pl.semaphore_signal(barrier, inc=1, device_id={"modes": my_block, "gz": part}, device_id_type=MESH)

            return 0

        lax.fori_loop(1, parts, signal_parts, 0)

    for copy in loads[1:]:
        copy.wait()
    low = [low_s[k] for k in range(rows)]
    up = [up_s[k] for k in range(rows)]
    low[0] = jnp.where(gi == 0, 0.0, low[0])
    up[last] = jnp.where(gi == parts - 1, 0.0, up[last])

    lane = lax.broadcasted_iota(jnp.int32, (2, LANES), 1)
    packed = jnp.zeros((2, LANES), jnp.float32)
    for k in range(rows):
        packed = jnp.where(lane == k, low[k], packed)
        packed = jnp.where(lane == rows + k, up[k], packed)
    CS[...] = packed

    for j in range(modes):
        for b in range(2):
            LAM[j, pl.ds(b, 1), :] = es_s[2 * j + b] + EP[pl.ds(mi, 1), :]
    lam = LAM[...]
    loads[0].wait()
    excess = lam + low[0]
    q = [None, None]
    for k in range(last):
        inv = 1.0 / (up[k] + excess)
        FAC[k] = up[k] * inv
        for c in range(2):
            q[c] = (F[k, c] if k == 0 else F[k, c] + low[k] * q[c]) * inv
            F[k, c] = q[c]
        excess = lam + low[k + 1] * (excess * inv)
    for c in range(2):
        SAB[c] = F[last, c] + low[last] * q[c]
    for k in range(last - 2, -1, -1):
        factor = FAC[k]
        for c in range(2):
            q[c] = F[k, c] + factor * q[c]
            F[k, c] = q[c]
    for c in range(2):
        SAB[2 + c] = q[c]

    def s_copy(target, slot):
        return pltpu.make_async_remote_copy(
            src_ref=SAB.at[:, target], dst_ref=AB.at[:, slot],
            send_sem=s_send.at[target], recv_sem=s_recv.at[slot],
            device_id={"modes": target}, device_id_type=MESH)

    def forward_copy(block, slot):
        return pltpu.make_async_remote_copy(
            src_ref=AB.at[:, block], dst_ref=GR.at[slot],
            send_sem=ab_send.at[block], recv_sem=ab_recv.at[slot],
            device_id={"gz": home(block)}, device_id_type=MESH)

    def direct_copy(target, slot):
        return pltpu.make_async_remote_copy(
            src_ref=SAB.at[:, target], dst_ref=GR.at[slot],
            send_sem=ab_send.at[target], recv_sem=ab_recv.at[slot],
            device_id={"modes": target, "gz": my_home}, device_id_type=MESH)

    def y_copy(target, slot):
        return pltpu.make_async_remote_copy(
            src_ref=F.at[pl.ds(0, last), :, target], dst_ref=W.at[:, :, slot],
            send_sem=y_send.at[target], recv_sem=y_recv.at[slot],
            device_id={"modes": target}, device_id_type=MESH)

    def c_copy(block, slot):
        return pltpu.make_async_remote_copy(
            src_ref=CS, dst_ref=CR.at[slot],
            send_sem=c_send.at[block], recv_sem=c_recv.at[slot],
            device_id={"gz": home(block)}, device_id_type=MESH)

    def r_copy(part, slot):
        return pltpu.make_async_remote_copy(
            src_ref=RS.at[part], dst_ref=XR.at[slot],
            send_sem=r_send.at[part], recv_sem=r_recv.at[slot],
            device_id={"gz": part}, device_id_type=MESH)

    solver_i = jnp.where(is_solver, 1, 0)
    late_i = jnp.where(is_late, modes, 0)
    pl.semaphore_wait(barrier, (modes - 1) + (modes - solver_i) + late_i)

    @pl.when(is_late)
    def _():
        def start_direct(i, _):
            direct_copy(lax.rem(mi + spread(i, modes // 2), modes), gi).start()
            return 0

        lax.fori_loop(0, modes, start_direct, 0)

    @pl.when(jnp.logical_not(is_late))
    def _():
        def start_s(i, _):
            s_copy(lax.rem(mi + spread(i, modes // 2), modes), mi).start()
            return 0

        lax.fori_loop(0, modes - 1, start_s, 0)
        AB[:, mi] = SAB[:, mi]

    def start_c(j, _):
        @pl.when(home(j) != gi)
        def _():
            c_copy(j, gi).start()

        return 0

    lax.fori_loop(0, modes, start_c, 0)

    def start_y(i, _):
        y_copy(lax.rem(mi + spread(i, modes // 2), modes), mi).start()
        return 0

    lax.fori_loop(0, modes - 1, start_y, 0)
    W[:, :, mi] = F[0:last, :, mi]

    for b in range(2):
        LAM[:, pl.ds(b, 1), :] = (es_s[mi * 2 + b] + EP[...]).reshape(modes, 1, LANES)
    lam = LAM[...]
    excess = lam + low[0]
    for k in range(last):
        inv = 1.0 / (up[k] + excess)
        factor = up[k] * inv
        v = low[0] * inv if k == 0 else (low[k] * inv) * v
        FAC[k] = factor
        V[k] = v
        excess = lam + low[k + 1] * (excess * inv)
    t = factor
    T[last - 1] = t
    for k in range(last - 2, -1, -1):
        factor = FAC[k]
        v = V[k] + factor * v
        t = factor * t
        V[k] = v
        T[k] = t

    @pl.when(jnp.logical_not(is_late))
    def _():
        def forward(i, _):
            r = modes - 1 - i
            block = spread(r // 2, half) * 2 + lax.rem(r, 2)

            @pl.when(block != mi)
            def _():
                s_copy(block, block).wait_recv()

            @pl.when(home(block) != gi)
            def _():
                forward_copy(block, gi).start()

            @pl.when(home(block) == gi)
            def _():
                GR[gi] = AB[:, block]

            return 0

        lax.fori_loop(0, modes, forward, 0)

    count = 2 * parts

    def ahead(x, d):
        return pltpu.roll(x, count - 2 * d, 0)

    def behind(x, d):
        return pltpu.roll(x, 2 * d, 0)

    def spread_lane(x, k):
        return jnp.broadcast_to(x[:, k:k + 1], (count, LANES))

    @pl.when(is_solver)
    def _():
        CR[gi] = CS[...]

        def wait_c(i, _):
            c_copy(my_block, lax.rem(gi + i, parts)).wait_recv()
            return 0

        lax.fori_loop(1, parts, wait_c, 0)
        PK[0] = CR[...].reshape(count, LANES)
        couplings = PK[0]
        odd = lax.rem(lax.broadcasted_iota(jnp.int32, (count, LANES), 0), 2) == 1
        stream = jnp.where(odd, es_s[mi * 2 + 1], es_s[mi * 2])
        lam = stream + jnp.broadcast_to(EP[pl.ds(my_block, 1), :], (count, LANES))
        for k in range(last):
            lo = spread_lane(couplings, k)
            hi = spread_lane(couplings, rows + k)
            excess = lam + lo if k == 0 else lam + lo * (excess * inv)
            inv = 1.0 / (hi + excess)
            factor = hi * inv
            if k == 0:
                v = lo * inv
                qh = lam * inv
                h = qh
                t = factor
            else:
                v = (lo * inv) * v
                qh = (lam + lo * qh) * inv
                h = h + t * qh
                t = t * factor
        lo = spread_lane(couplings, last)
        u = spread_lane(couplings, rows + last)
        a = lo * v
        c = u * ahead(t, 1)
        e = lam + lo * qh + u * ahead(h, 1)
        d, level = 1, 0
        while d < parts:
            inv = 1.0 / (a + c + e)
            alpha = a * behind(inv, d)
            gamma = c * ahead(inv, d)
            AL[level] = alpha
            GA[level] = gamma
            e = e + alpha * behind(e, d) + gamma * ahead(e, d)
            a = alpha * behind(a, d)
            c = gamma * ahead(c, d)
            d, level = 2 * d, level + 1
        EI[...] = 1.0 / e

        def wait_ab(part, _):
            @pl.when(part != gi)
            def _():
                direct_copy(mi, part).wait_recv()

            return 0

        lax.fori_loop(0, parts, wait_ab, 0)
        for p in range(2):
            PK[0] = GR[:, p].reshape(count, LANES)
            PK[1] = GR[:, 2 + p].reshape(count, LANES)
            x = PK[0] + u * ahead(PK[1], 1)
            d, level = 1, 0
            while d < parts:
                x = x + AL[level] * behind(x, d) + GA[level] * ahead(x, d)
                d, level = 2 * d, level + 1
            x = x * EI[...]
            RS[:, 1, p] = x.reshape(parts, 2, LANES)
            RS[:, 0, p] = behind(x, 1).reshape(parts, 2, LANES)

        def start_r(i, _):
            part = lax.rem(i, cols) * depth + i // cols

            @pl.when(part != gi)
            def _():
                r_copy(part, my_block).start()

            return 0

        lax.fori_loop(0, parts, start_r, 0)
        XR[my_block] = RS[gi]

    def wait_y(i, _):
        slot = lax.rem(mi + i, modes)
        y_copy(slot, slot).wait_recv()
        return 0

    lax.fori_loop(1, modes, wait_y, 0)

    def finish_modes(i, _):
        target = lax.rem(mi + i, modes)
        y_copy(target, target).wait_send()
        return 0

    lax.fori_loop(1, modes, finish_modes, 0)

    def finish_solvers(j, _):
        @pl.when(home(j) != gi)
        def _():
            c_copy(j, gi).wait_send()
            forward_copy(j, gi).wait_send()

        return 0

    lax.fori_loop(0, modes, finish_solvers, 0)

    @pl.when(jnp.logical_not(is_late))
    def _():
        def finish_s(i, _):
            target = lax.rem(mi + i, modes)
            s_copy(target, target).wait_send()
            return 0

        lax.fori_loop(1, modes, finish_s, 0)

    @pl.when(is_solver)
    def _():
        def finish_r(i, _):
            r_copy(lax.rem(gi + i, parts), my_block).wait_send()
            return 0

        lax.fori_loop(1, parts, finish_r, 0)

    def wait_r(j, _):
        @pl.when(home(j) != gi)
        def _():
            r_copy(gi, j).wait_recv()

        return 0

    lax.fori_loop(0, modes, wait_r, 0)


def combine_kernel(W, XR, V, T, out_hbm, O, store_sem):
    rows, modes = O.shape[0], V.shape[1]
    last = rows - 1
    stores = [pltpu.make_async_copy(O.at[k], out_hbm.at[k], store_sem.at[k]) for k in range(rows)]
    for k in range(rows):
        for p in range(2):
            own = XR[:, 1, p]
            value = own if k == last else W[k, p] + V[k] * XR[:, 0, p] + T[k] * own
            for j in range(modes):
                O[k, p, :, pl.ds(j * LANES, LANES)] = value[j]
        stores[k].start()
    for copy in stores:
        copy.wait()


def solution(mesh):
    modes, parts = mesh.shape["modes"], mesh.shape["gz"]

    def per_device(source_field, coupling_below, coupling_above, eigen_stream, eigen_span):
        rows, _, kx, _ = source_field.shape
        levels = (parts - 1).bit_length()
        f32 = jnp.float32
        tile = (2, LANES)
        vmem = lambda *shape: pltpu.VMEM(shape + tile, f32)
        flat = lambda *shape: pltpu.VMEM(shape + (2 * parts, LANES), f32)
        dma = lambda *shape: pltpu.SemaphoreType.DMA(shape)
        smem = lambda n: pltpu.SMEM((n,), f32)
        anywhere = pl.BlockSpec(memory_space=pl.ANY)
        local = pl.BlockSpec(memory_space=pltpu.VMEM)
        arrived = pl.pallas_call(
            functools.partial(exchange_kernel, modes, parts),
            out_shape=[
                vmem(rows - 1, 2, modes), vmem(modes, 2, 2), vmem(rows - 1, modes), vmem(rows - 1, modes),
            ],
            in_specs=[anywhere] * 5,
            out_specs=[local] * 4,
            scratch_shapes=[
                vmem(rows, 2, modes),
                vmem(4, modes), vmem(4, modes), vmem(), vmem(parts), vmem(parts, 4), vmem(parts, 2, 2),
                vmem(rows - 1, modes),
                flat(levels), flat(levels), flat(), flat(2), vmem(modes),
                pltpu.VMEM((modes, LANES), f32), smem(rows), smem(rows), smem(kx),
                dma(5), dma(modes), dma(modes), dma(modes), dma(modes),
                dma(modes), dma(parts), dma(modes), dma(parts), dma(parts), dma(modes),
            ],
            compiler_params=pltpu.CompilerParams(collective_id=0, has_side_effects=True),
        )(
            source_field.reshape(rows, 2, modes, 2, LANES),
            coupling_below, coupling_above, eigen_stream, eigen_span.reshape(modes, LANES),
        )
        return pl.pallas_call(
            combine_kernel,
            out_shape=jax.ShapeDtypeStruct((rows, 2, kx // modes, modes * LANES), f32),
            in_specs=[local] * 4,
            out_specs=anywhere,
            scratch_shapes=[pltpu.VMEM((rows, 2, kx // modes, modes * LANES), f32), dma(rows)],
            compiler_params=pltpu.CompilerParams(vmem_limit_bytes=4 << 20),
        )(*[pltpu.with_memory_space_constraint(x, pltpu.VMEM) for x in arrived])

    return jax.shard_map(
        per_device,
        mesh=mesh,
        in_specs=(P("gz", None, None, "modes"), P("gz"), P("gz"), P(), P()),
        out_specs=P("gz", None, "modes", None),
        check_vma=False,
    )
```

```python
import functools

import jax
import jax.numpy as jnp
from jax import lax
from jax.experimental import pallas as pl
from jax.experimental.pallas import tpu as pltpu
from jax.sharding import PartitionSpec as P

MESH = pl.DeviceIdType.MESH
LANES = 128


def gz_columns(parts):
    return min(4, parts // 2)


def spread(i, half):
    return jnp.where(lax.rem(i, 2) == 0, half + i // 2, half - (i + 1) // 2)


def exchange_kernel(
    modes, parts,
    f_hbm, low_hbm, up_hbm, es_hbm, ep_hbm,
    W, XR, V, T,
    F, SAB, AB, CS, CR, GR, RS, FAC, AL, GA, EI, PK, LAM, EP, low_s, up_s, es_s,
    load_sem, y_send, y_recv, s_send, s_recv, ab_send, ab_recv, c_send, c_recv, r_send, r_recv,
):
    rows = F.shape[0]
    last = rows - 1
    half = modes // 4
    cols = gz_columns(parts)
    depth = parts // cols
    mi = lax.axis_index("modes")
    gi = lax.axis_index("gz")

    moved = (modes - 2, 4) if (modes, parts) == (16, 32) else None

    def home(j):
        d = j // 2 - half
        r = jnp.where(d > 0, 2 * d, jnp.where(d < 0, -2 * d - 1, 0)) * 2 + lax.rem(j, 2)
        site = lax.rem(r, cols) * depth + r // cols
        return jnp.where(r == moved[0], moved[1], site) if moved else site

    rank = lax.rem(gi, depth) * cols + gi // depth
    if moved:
        rank = jnp.where(gi == moved[1], moved[0], jnp.where(rank == moved[0], modes, rank))
    is_solver = rank < modes
    my_block = spread(jnp.minimum(rank, modes - 1) // 2, half) * 2 + lax.rem(rank, 2)
    my_home = home(mi)
    def late(part):
        z_late = lax.rem(part, depth) >= depth // 2
        return jnp.logical_and(z_late, part != moved[1]) if moved else z_late

    is_late = late(gi)

    loads = [
        pltpu.make_async_copy(src, dst, load_sem.at[i])
        for i, (src, dst) in enumerate(
            [(f_hbm, F), (low_hbm, low_s), (up_hbm, up_s), (es_hbm, es_s), (ep_hbm, EP)])
    ]
    for copy in loads:
        copy.start()

    barrier = pltpu.get_barrier_semaphore()

    def signal_modes(r, _):
        pl.semaphore_signal(barrier, inc=1, device_id={"modes": lax.rem(mi + r, modes)}, device_id_type=MESH)
        return 0

    lax.fori_loop(1, modes, signal_modes, 0)

    @pl.when(is_solver)
    def _():
        def signal_parts(r, _):
            part = lax.rem(gi + r, parts)
            pl.semaphore_signal(barrier, inc=1, device_id={"gz": part}, device_id_type=MESH)

            @pl.when(late(part))
            def _():
                pl.semaphore_signal(barrier, inc=1, device_id={"modes": my_block, "gz": part}, device_id_type=MESH)

            return 0

        lax.fori_loop(1, parts, signal_parts, 0)

    for copy in loads[1:]:
        copy.wait()
    low = [low_s[k] for k in range(rows)]
    up = [up_s[k] for k in range(rows)]
    low[0] = jnp.where(gi == 0, 0.0, low[0])
    up[last] = jnp.where(gi == parts - 1, 0.0, up[last])

    lane = lax.broadcasted_iota(jnp.int32, (2, LANES), 1)
    packed = jnp.zeros((2, LANES), jnp.float32)
    for k in range(rows):
        packed = jnp.where(lane == k, low[k], packed)
        packed = jnp.where(lane == rows + k, up[k], packed)
    CS[...] = packed

    for j in range(modes):
        for b in range(2):
            LAM[j, pl.ds(b, 1), :] = es_s[2 * j + b] + EP[pl.ds(mi, 1), :]
    lam = LAM[...]
    loads[0].wait()
    excess = lam + low[0]
    q = [None, None]
    for k in range(last):
        inv = 1.0 / (up[k] + excess)
        FAC[k] = up[k] * inv
        for c in range(2):
            q[c] = (F[k, c] if k == 0 else F[k, c] + low[k] * q[c]) * inv
            F[k, c] = q[c]
        excess = lam + low[k + 1] * (excess * inv)
    for c in range(2):
        SAB[c] = F[last, c] + low[last] * q[c]
    for k in range(last - 2, -1, -1):
        factor = FAC[k]
        for c in range(2):
            q[c] = F[k, c] + factor * q[c]
            F[k, c] = q[c]
    for c in range(2):
        SAB[2 + c] = q[c]

    def s_copy(target, slot):
        return pltpu.make_async_remote_copy(
            src_ref=SAB.at[:, target], dst_ref=AB.at[:, slot],
            send_sem=s_send.at[target], recv_sem=s_recv.at[slot],
            device_id={"modes": target}, device_id_type=MESH)

    def forward_copy(block, slot):
        return pltpu.make_async_remote_copy(
            src_ref=AB.at[:, block], dst_ref=GR.at[slot],
            send_sem=ab_send.at[block], recv_sem=ab_recv.at[slot],
            device_id={"gz": home(block)}, device_id_type=MESH)

    def direct_copy(target, slot):
        return pltpu.make_async_remote_copy(
            src_ref=SAB.at[:, target], dst_ref=GR.at[slot],
            send_sem=ab_send.at[target], recv_sem=ab_recv.at[slot],
            device_id={"modes": target, "gz": my_home}, device_id_type=MESH)

    def y_copy(target, slot):
        return pltpu.make_async_remote_copy(
            src_ref=F.at[pl.ds(0, last), :, target], dst_ref=W.at[:, :, slot],
            send_sem=y_send.at[target], recv_sem=y_recv.at[slot],
            device_id={"modes": target}, device_id_type=MESH)

    def c_copy(block, slot):
        return pltpu.make_async_remote_copy(
            src_ref=CS, dst_ref=CR.at[slot],
            send_sem=c_send.at[block], recv_sem=c_recv.at[slot],
            device_id={"gz": home(block)}, device_id_type=MESH)

    def r_copy(part, slot):
        return pltpu.make_async_remote_copy(
            src_ref=RS.at[part], dst_ref=XR.at[slot],
            send_sem=r_send.at[part], recv_sem=r_recv.at[slot],
            device_id={"gz": part}, device_id_type=MESH)

    solver_i = jnp.where(is_solver, 1, 0)
    late_i = jnp.where(is_late, modes, 0)
    pl.semaphore_wait(barrier, (modes - 1) + (modes - solver_i) + late_i)

    @pl.when(is_late)
    def _():
        def start_direct(i, _):
            direct_copy(lax.rem(mi + spread(i, modes // 2), modes), gi).start()
            return 0

        lax.fori_loop(0, modes, start_direct, 0)

    @pl.when(jnp.logical_not(is_late))
    def _():
        def start_s(i, _):
            s_copy(lax.rem(mi + spread(i, modes // 2), modes), mi).start()
            return 0

        lax.fori_loop(0, modes - 1, start_s, 0)
        AB[:, mi] = SAB[:, mi]

    def start_c(j, _):
        @pl.when(home(j) != gi)
        def _():
            c_copy(j, gi).start()

        return 0

    lax.fori_loop(0, modes, start_c, 0)

    def start_y(i, _):
        y_copy(lax.rem(mi + spread(i, modes // 2), modes), mi).start()
        return 0

    @pl.when(jnp.logical_not(is_late))
    def _():
        lax.fori_loop(0, modes - 1, start_y, 0)

    W[:, :, mi] = F[0:last, :, mi]

    for b in range(2):
        LAM[:, pl.ds(b, 1), :] = (es_s[mi * 2 + b] + EP[...]).reshape(modes, 1, LANES)
    lam = LAM[...]
    excess = lam + low[0]
    for k in range(last):
        inv = 1.0 / (up[k] + excess)
        factor = up[k] * inv
        v = low[0] * inv if k == 0 else (low[k] * inv) * v
        FAC[k] = factor
        V[k] = v
        excess = lam + low[k + 1] * (excess * inv)
    t = factor
    T[last - 1] = t
    for k in range(last - 2, -1, -1):
        factor = FAC[k]
        v = V[k] + factor * v
        t = factor * t
        V[k] = v
        T[k] = t

    @pl.when(is_late)
    def _():
        lax.fori_loop(0, modes - 1, start_y, 0)

    @pl.when(jnp.logical_not(is_late))
    def _():
        def forward(i, _):
            r = modes - 1 - i
            block = spread(r // 2, half) * 2 + lax.rem(r, 2)

            @pl.when(block != mi)
            def _():
                s_copy(block, block).wait_recv()

            @pl.when(home(block) != gi)
            def _():
                forward_copy(block, gi).start()

            @pl.when(home(block) == gi)
            def _():
                GR[gi] = AB[:, block]

            return 0

        lax.fori_loop(0, modes, forward, 0)

    count = 2 * parts

    def ahead(x, d):
        return pltpu.roll(x, count - 2 * d, 0)

    def behind(x, d):
        return pltpu.roll(x, 2 * d, 0)

    def spread_lane(x, k):
        return jnp.broadcast_to(x[:, k:k + 1], (count, LANES))

    @pl.when(is_solver)
    def _():
        CR[gi] = CS[...]

        def wait_c(i, _):
            c_copy(my_block, lax.rem(gi + i, parts)).wait_recv()
            return 0

        lax.fori_loop(1, parts, wait_c, 0)
        PK[0] = CR[...].reshape(count, LANES)
        couplings = PK[0]
        odd = lax.rem(lax.broadcasted_iota(jnp.int32, (count, LANES), 0), 2) == 1
        stream = jnp.where(odd, es_s[mi * 2 + 1], es_s[mi * 2])
        lam = stream + jnp.broadcast_to(EP[pl.ds(my_block, 1), :], (count, LANES))
        for k in range(last):
            lo = spread_lane(couplings, k)
            hi = spread_lane(couplings, rows + k)
            excess = lam + lo if k == 0 else lam + lo * (excess * inv)
            inv = 1.0 / (hi + excess)
            factor = hi * inv
            if k == 0:
                v = lo * inv
                qh = lam * inv
                h = qh
                t = factor
            else:
                v = (lo * inv) * v
                qh = (lam + lo * qh) * inv
                h = h + t * qh
                t = t * factor
        lo = spread_lane(couplings, last)
        u = spread_lane(couplings, rows + last)
        a = lo * v
        c = u * ahead(t, 1)
        e = lam + lo * qh + u * ahead(h, 1)
        d, level = 1, 0
        while d < parts:
            inv = 1.0 / (a + c + e)
            alpha = a * behind(inv, d)
            gamma = c * ahead(inv, d)
            AL[level] = alpha
            GA[level] = gamma
            e = e + alpha * behind(e, d) + gamma * ahead(e, d)
            a = alpha * behind(a, d)
            c = gamma * ahead(c, d)
            d, level = 2 * d, level + 1
        EI[...] = 1.0 / e

        def wait_ab(part, _):
            @pl.when(part != gi)
            def _():
                direct_copy(mi, part).wait_recv()

            return 0

        lax.fori_loop(0, parts, wait_ab, 0)
        for p in range(2):
            PK[0] = GR[:, p].reshape(count, LANES)
            PK[1] = GR[:, 2 + p].reshape(count, LANES)
            x = PK[0] + u * ahead(PK[1], 1)
            d, level = 1, 0
            while d < parts:
                x = x + AL[level] * behind(x, d) + GA[level] * ahead(x, d)
                d, level = 2 * d, level + 1
            x = x * EI[...]
            RS[:, 1, p] = x.reshape(parts, 2, LANES)
            RS[:, 0, p] = behind(x, 1).reshape(parts, 2, LANES)

        def start_r(i, _):
            part = lax.rem(i, cols) * depth + i // cols

            @pl.when(part != gi)
            def _():
                r_copy(part, my_block).start()

            return 0

        lax.fori_loop(0, parts, start_r, 0)
        XR[my_block] = RS[gi]

    def wait_y(i, _):
        slot = lax.rem(mi + i, modes)
        y_copy(slot, slot).wait_recv()
        return 0

    lax.fori_loop(1, modes, wait_y, 0)

    def finish_modes(i, _):
        target = lax.rem(mi + i, modes)
        y_copy(target, target).wait_send()
        return 0

    lax.fori_loop(1, modes, finish_modes, 0)

    def finish_solvers(j, _):
        @pl.when(home(j) != gi)
        def _():
            c_copy(j, gi).wait_send()
            forward_copy(j, gi).wait_send()

        return 0

    lax.fori_loop(0, modes, finish_solvers, 0)

    @pl.when(jnp.logical_not(is_late))
    def _():
        def finish_s(i, _):
            target = lax.rem(mi + i, modes)
            s_copy(target, target).wait_send()
            return 0

        lax.fori_loop(1, modes, finish_s, 0)

    @pl.when(is_solver)
    def _():
        def finish_r(i, _):
            r_copy(lax.rem(gi + i, parts), my_block).wait_send()
            return 0

        lax.fori_loop(1, parts, finish_r, 0)

    def wait_r(j, _):
        @pl.when(home(j) != gi)
        def _():
            r_copy(gi, j).wait_recv()

        return 0

    lax.fori_loop(0, modes, wait_r, 0)


def combine_kernel(W, XR, V, T, out_hbm, O, store_sem):
    rows, modes = O.shape[0], V.shape[1]
    last = rows - 1
    chunk = 4
    stores = [
        pltpu.make_async_copy(O.at[pl.ds(k, chunk)], out_hbm.at[pl.ds(k, chunk)], store_sem.at[k // chunk])
        for k in range(0, rows, chunk)
    ]
    for k in range(rows):
        for p in range(2):
            own = XR[:, 1, p]
            value = own if k == last else W[k, p] + V[k] * XR[:, 0, p] + T[k] * own
            for j in range(modes):
                O[k, p, :, pl.ds(j * LANES, LANES)] = value[j]
        if k % chunk == chunk - 1:
            stores[k // chunk].start()
    for copy in stores:
        copy.wait()


def solution(mesh):
    modes, parts = mesh.shape["modes"], mesh.shape["gz"]

    def per_device(source_field, coupling_below, coupling_above, eigen_stream, eigen_span):
        rows, _, kx, _ = source_field.shape
        levels = (parts - 1).bit_length()
        f32 = jnp.float32
        tile = (2, LANES)
        vmem = lambda *shape: pltpu.VMEM(shape + tile, f32)
        flat = lambda *shape: pltpu.VMEM(shape + (2 * parts, LANES), f32)
        dma = lambda *shape: pltpu.SemaphoreType.DMA(shape)
        smem = lambda n: pltpu.SMEM((n,), f32)
        anywhere = pl.BlockSpec(memory_space=pl.ANY)
        local = pl.BlockSpec(memory_space=pltpu.VMEM)
        arrived = pl.pallas_call(
            functools.partial(exchange_kernel, modes, parts),
            out_shape=[
                vmem(rows - 1, 2, modes), vmem(modes, 2, 2), vmem(rows - 1, modes), vmem(rows - 1, modes),
            ],
            in_specs=[anywhere] * 5,
            out_specs=[local] * 4,
            scratch_shapes=[
                vmem(rows, 2, modes),
                vmem(4, modes), vmem(4, modes), vmem(), vmem(parts), vmem(parts, 4), vmem(parts, 2, 2),
                vmem(rows - 1, modes),
                flat(levels), flat(levels), flat(), flat(2), vmem(modes),
                pltpu.VMEM((modes, LANES), f32), smem(rows), smem(rows), smem(kx),
                dma(5), dma(modes), dma(modes), dma(modes), dma(modes),
                dma(modes), dma(parts), dma(modes), dma(parts), dma(parts), dma(modes),
            ],
            compiler_params=pltpu.CompilerParams(collective_id=0, has_side_effects=True),
        )(
            source_field.reshape(rows, 2, modes, 2, LANES),
            coupling_below, coupling_above, eigen_stream, eigen_span.reshape(modes, LANES),
        )
        return pl.pallas_call(
            combine_kernel,
            out_shape=jax.ShapeDtypeStruct((rows, 2, kx // modes, modes * LANES), f32),
            in_specs=[local] * 4,
            out_specs=anywhere,
            scratch_shapes=[pltpu.VMEM((rows, 2, kx // modes, modes * LANES), f32), dma(rows // 4)],
            compiler_params=pltpu.CompilerParams(vmem_limit_bytes=4 << 20),
        )(*[pltpu.with_memory_space_constraint(x, pltpu.VMEM) for x in arrived])

    return jax.shard_map(
        per_device,
        mesh=mesh,
        in_specs=(P("gz", None, None, "modes"), P("gz"), P("gz"), P(), P()),
        out_specs=P("gz", None, "modes", None),
        check_vma=False,
    )
```

```python
import functools

import jax
import jax.numpy as jnp
from jax import lax
from jax.experimental import pallas as pl
from jax.experimental.pallas import tpu as pltpu
from jax.sharding import PartitionSpec as P

MESH = pl.DeviceIdType.MESH
LANES = 128


def gz_columns(parts):
    return min(4, parts // 2)


def spread(i, half):
    return jnp.where(lax.rem(i, 2) == 0, half + i // 2, half - (i + 1) // 2)


def exchange_kernel(
    modes, parts,
    f_hbm, low_hbm, up_hbm, es_hbm, ep_hbm,
    W, XR, V, T,
    F, SAB, AB, CS, CR, GR, RS, FAC, AL, GA, EI, PK, LAM, EP, low_s, up_s, es_s,
    load_sem, y_send, y_recv, s_send, s_recv, ab_send, ab_recv, c_send, c_recv, r_send, r_recv,
):
    rows = F.shape[0]
    last = rows - 1
    half = modes // 4
    cols = gz_columns(parts)
    depth = parts // cols
    mi = lax.axis_index("modes")
    gi = lax.axis_index("gz")

    moved = (modes - 2, 4) if (modes, parts) == (16, 32) else None

    def home(j):
        d = j // 2 - half
        r = jnp.where(d > 0, 2 * d, jnp.where(d < 0, -2 * d - 1, 0)) * 2 + lax.rem(j, 2)
        site = lax.rem(r, cols) * depth + r // cols
        return jnp.where(r == moved[0], moved[1], site) if moved else site

    rank = lax.rem(gi, depth) * cols + gi // depth
    if moved:
        rank = jnp.where(gi == moved[1], moved[0], jnp.where(rank == moved[0], modes, rank))
    is_solver = rank < modes
    my_block = spread(jnp.minimum(rank, modes - 1) // 2, half) * 2 + lax.rem(rank, 2)
    my_home = home(mi)
    def late(part):
        z_late = lax.rem(part, depth) >= depth // 2
        return jnp.logical_and(z_late, part != moved[1]) if moved else z_late

    is_late = late(gi)

    loads = [
        pltpu.make_async_copy(src, dst, load_sem.at[i])
        for i, (src, dst) in enumerate(
            [(f_hbm, F), (low_hbm, low_s), (up_hbm, up_s), (es_hbm, es_s), (ep_hbm, EP)])
    ]
    for copy in loads:
        copy.start()

    barrier = pltpu.get_barrier_semaphore()

    def signal_modes(r, _):
        pl.semaphore_signal(barrier, inc=1, device_id={"modes": lax.rem(mi + r, modes)}, device_id_type=MESH)
        return 0

    lax.fori_loop(1, modes, signal_modes, 0)

    @pl.when(is_solver)
    def _():
        def signal_parts(r, _):
            part = lax.rem(gi + r, parts)
            pl.semaphore_signal(barrier, inc=1, device_id={"gz": part}, device_id_type=MESH)

            @pl.when(late(part))
            def _():
                pl.semaphore_signal(barrier, inc=1, device_id={"modes": my_block, "gz": part}, device_id_type=MESH)

            return 0

        lax.fori_loop(1, parts, signal_parts, 0)

    for copy in loads[1:]:
        copy.wait()
    low = [low_s[k] for k in range(rows)]
    up = [up_s[k] for k in range(rows)]
    low[0] = jnp.where(gi == 0, 0.0, low[0])
    up[last] = jnp.where(gi == parts - 1, 0.0, up[last])

    lane = lax.broadcasted_iota(jnp.int32, (2, LANES), 1)
    packed = jnp.zeros((2, LANES), jnp.float32)
    for k in range(rows):
        packed = jnp.where(lane == k, low[k], packed)
        packed = jnp.where(lane == rows + k, up[k], packed)
    CS[...] = packed

    for j in range(modes):
        for b in range(2):
            LAM[j, pl.ds(b, 1), :] = es_s[2 * j + b] + EP[pl.ds(mi, 1), :]
    lam = LAM[...]
    loads[0].wait()
    excess = lam + low[0]
    q = [None, None]
    for k in range(last):
        inv = 1.0 / (up[k] + excess)
        FAC[k] = up[k] * inv
        for c in range(2):
            q[c] = (F[k, c] if k == 0 else F[k, c] + low[k] * q[c]) * inv
            F[k, c] = q[c]
        excess = lam + low[k + 1] * (excess * inv)
    for c in range(2):
        SAB[c] = F[last, c] + low[last] * q[c]
    for k in range(last - 2, -1, -1):
        factor = FAC[k]
        for c in range(2):
            q[c] = F[k, c] + factor * q[c]
            F[k, c] = q[c]
    for c in range(2):
        SAB[2 + c] = q[c]

    def s_copy(target, slot):
        return pltpu.make_async_remote_copy(
            src_ref=SAB.at[:, target], dst_ref=AB.at[:, slot],
            send_sem=s_send.at[target], recv_sem=s_recv.at[slot],
            device_id={"modes": target}, device_id_type=MESH)

    def forward_copy(block, slot):
        return pltpu.make_async_remote_copy(
            src_ref=AB.at[:, block], dst_ref=GR.at[slot],
            send_sem=ab_send.at[block], recv_sem=ab_recv.at[slot],
            device_id={"gz": home(block)}, device_id_type=MESH)

    def direct_copy(target, slot):
        return pltpu.make_async_remote_copy(
            src_ref=SAB.at[:, target], dst_ref=GR.at[slot],
            send_sem=ab_send.at[target], recv_sem=ab_recv.at[slot],
            device_id={"modes": target, "gz": my_home}, device_id_type=MESH)

    def y_copy(target, slot):
        return pltpu.make_async_remote_copy(
            src_ref=F.at[pl.ds(0, last), :, target], dst_ref=W.at[:, :, slot],
            send_sem=y_send.at[target], recv_sem=y_recv.at[slot],
            device_id={"modes": target}, device_id_type=MESH)

    def c_copy(block, slot):
        return pltpu.make_async_remote_copy(
            src_ref=CS, dst_ref=CR.at[slot],
            send_sem=c_send.at[block], recv_sem=c_recv.at[slot],
            device_id={"gz": home(block)}, device_id_type=MESH)

    def r_copy(part, slot):
        return pltpu.make_async_remote_copy(
            src_ref=RS.at[part], dst_ref=XR.at[slot],
            send_sem=r_send.at[part], recv_sem=r_recv.at[slot],
            device_id={"gz": part}, device_id_type=MESH)

    solver_i = jnp.where(is_solver, 1, 0)
    late_i = jnp.where(is_late, modes, 0)
    pl.semaphore_wait(barrier, (modes - 1) + (modes - solver_i) + late_i)

    @pl.when(is_late)
    def _():
        def start_direct(i, _):
            direct_copy(lax.rem(mi + spread(i, modes // 2), modes), gi).start()
            return 0

        lax.fori_loop(0, modes, start_direct, 0)

    @pl.when(jnp.logical_not(is_late))
    def _():
        def start_s(i, _):
            s_copy(lax.rem(mi + spread(i, modes // 2), modes), mi).start()
            return 0

        lax.fori_loop(0, modes - 1, start_s, 0)
        AB[:, mi] = SAB[:, mi]

    def start_c(j, _):
        @pl.when(home(j) != gi)
        def _():
            c_copy(j, gi).start()

        return 0

    lax.fori_loop(0, modes, start_c, 0)

    def start_y(i, _):
        y_copy(lax.rem(mi + spread(i, modes // 2), modes), mi).start()
        return 0

    @pl.when(jnp.logical_not(is_late))
    def _():
        lax.fori_loop(0, modes - 1, start_y, 0)

    W[:, :, mi] = F[0:last, :, mi]

    for b in range(2):
        LAM[:, pl.ds(b, 1), :] = (es_s[mi * 2 + b] + EP[...]).reshape(modes, 1, LANES)
    lam = LAM[...]
    excess = lam + low[0]
    for k in range(last):
        inv = 1.0 / (up[k] + excess)
        factor = up[k] * inv
        v = low[0] * inv if k == 0 else (low[k] * inv) * v
        FAC[k] = factor
        V[k] = v
        excess = lam + low[k + 1] * (excess * inv)
    t = factor
    T[last - 1] = t
    for k in range(last - 2, -1, -1):
        factor = FAC[k]
        v = V[k] + factor * v
        t = factor * t
        V[k] = v
        T[k] = t

    @pl.when(is_late)
    def _():
        lax.fori_loop(0, modes - 1, start_y, 0)

    @pl.when(jnp.logical_not(is_late))
    def _():
        def forward(i, _):
            r = modes - 1 - i
            block = spread(r // 2, half) * 2 + lax.rem(r, 2)

            @pl.when(block != mi)
            def _():
                s_copy(block, block).wait_recv()

            @pl.when(home(block) != gi)
            def _():
                forward_copy(block, gi).start()

            @pl.when(home(block) == gi)
            def _():
                GR[gi] = AB[:, block]

            return 0

        lax.fori_loop(0, modes, forward, 0)

    count = 2 * parts

    def ahead(x, d):
        return pltpu.roll(x, count - 2 * d, 0)

    def behind(x, d):
        return pltpu.roll(x, 2 * d, 0)

    def spread_lane(x, k):
        return jnp.broadcast_to(x[:, k:k + 1], (count, LANES))

    @pl.when(is_solver)
    def _():
        CR[gi] = CS[...]

        def wait_c(i, _):
            c_copy(my_block, lax.rem(gi + i, parts)).wait_recv()
            return 0

        lax.fori_loop(1, parts, wait_c, 0)
        PK[0] = CR[...].reshape(count, LANES)
        couplings = PK[0]
        odd = lax.rem(lax.broadcasted_iota(jnp.int32, (count, LANES), 0), 2) == 1
        stream = jnp.where(odd, es_s[mi * 2 + 1], es_s[mi * 2])
        lam = stream + jnp.broadcast_to(EP[pl.ds(my_block, 1), :], (count, LANES))
        for k in range(last):
            lo = spread_lane(couplings, k)
            hi = spread_lane(couplings, rows + k)
            excess = lam + lo if k == 0 else lam + lo * (excess * inv)
            inv = 1.0 / (hi + excess)
            factor = hi * inv
            if k == 0:
                v = lo * inv
                qh = lam * inv
                h = qh
                t = factor
            else:
                v = (lo * inv) * v
                qh = (lam + lo * qh) * inv
                h = h + t * qh
                t = t * factor
        lo = spread_lane(couplings, last)
        u = spread_lane(couplings, rows + last)
        a = lo * v
        c = u * ahead(t, 1)
        e = lam + lo * qh + u * ahead(h, 1)
        d, level = 1, 0
        while d < parts:
            inv = 1.0 / (a + c + e)
            alpha = a * behind(inv, d)
            gamma = c * ahead(inv, d)
            AL[level] = alpha
            GA[level] = gamma
            e = e + alpha * behind(e, d) + gamma * ahead(e, d)
            a = alpha * behind(a, d)
            c = gamma * ahead(c, d)
            d, level = 2 * d, level + 1
        EI[...] = 1.0 / e

        def wait_ab(part, _):
            @pl.when(part != gi)
            def _():
                direct_copy(mi, part).wait_recv()

            return 0

        lax.fori_loop(0, parts, wait_ab, 0)
        for p in range(2):
            PK[0] = GR[:, p].reshape(count, LANES)
            PK[1] = GR[:, 2 + p].reshape(count, LANES)
            x = PK[0] + u * ahead(PK[1], 1)
            d, level = 1, 0
            while d < parts:
                x = x + AL[level] * behind(x, d) + GA[level] * ahead(x, d)
                d, level = 2 * d, level + 1
            x = x * EI[...]
            RS[:, 1, p] = x.reshape(parts, 2, LANES)
            RS[:, 0, p] = behind(x, 1).reshape(parts, 2, LANES)

        def start_r(i, _):
            part = lax.rem(i, cols) * depth + i // cols

            @pl.when(part != gi)
            def _():
                r_copy(part, my_block).start()

            return 0

        lax.fori_loop(0, parts, start_r, 0)
        XR[my_block] = RS[gi]

    def wait_y(i, _):
        slot = lax.rem(mi + i, modes)
        y_copy(slot, slot).wait_recv()
        return 0

    lax.fori_loop(1, modes, wait_y, 0)

    def finish_modes(i, _):
        target = lax.rem(mi + i, modes)
        y_copy(target, target).wait_send()
        return 0

    lax.fori_loop(1, modes, finish_modes, 0)

    def finish_solvers(j, _):
        @pl.when(home(j) != gi)
        def _():
            c_copy(j, gi).wait_send()
            forward_copy(j, gi).wait_send()

        return 0

    lax.fori_loop(0, modes, finish_solvers, 0)

    @pl.when(jnp.logical_not(is_late))
    def _():
        def finish_s(i, _):
            target = lax.rem(mi + i, modes)
            s_copy(target, target).wait_send()
            return 0

        lax.fori_loop(1, modes, finish_s, 0)

    @pl.when(is_solver)
    def _():
        def finish_r(i, _):
            r_copy(lax.rem(gi + i, parts), my_block).wait_send()
            return 0

        lax.fori_loop(1, parts, finish_r, 0)

    def wait_r(j, _):
        @pl.when(home(j) != gi)
        def _():
            r_copy(gi, j).wait_recv()

        return 0

    lax.fori_loop(0, modes, wait_r, 0)


def combine_kernel(W, XR, V, T, out_hbm, O, store_sem):
    rows, modes = O.shape[0], V.shape[1]
    last = rows - 1
    chunk = 8
    stores = [
        pltpu.make_async_copy(O.at[pl.ds(k, chunk)], out_hbm.at[pl.ds(k, chunk)], store_sem.at[k // chunk])
        for k in range(0, rows, chunk)
    ]
    for k in range(rows):
        for p in range(2):
            own = XR[:, 1, p]
            value = own if k == last else W[k, p] + V[k] * XR[:, 0, p] + T[k] * own
            for j in range(modes):
                O[k, p, :, pl.ds(j * LANES, LANES)] = value[j]
        if k % chunk == chunk - 1:
            stores[k // chunk].start()
    for copy in stores:
        copy.wait()


def solution(mesh):
    modes, parts = mesh.shape["modes"], mesh.shape["gz"]

    def per_device(source_field, coupling_below, coupling_above, eigen_stream, eigen_span):
        rows, _, kx, _ = source_field.shape
        levels = (parts - 1).bit_length()
        f32 = jnp.float32
        tile = (2, LANES)
        vmem = lambda *shape: pltpu.VMEM(shape + tile, f32)
        flat = lambda *shape: pltpu.VMEM(shape + (2 * parts, LANES), f32)
        dma = lambda *shape: pltpu.SemaphoreType.DMA(shape)
        smem = lambda n: pltpu.SMEM((n,), f32)
        anywhere = pl.BlockSpec(memory_space=pl.ANY)
        local = pl.BlockSpec(memory_space=pltpu.VMEM)
        arrived = pl.pallas_call(
            functools.partial(exchange_kernel, modes, parts),
            out_shape=[
                vmem(rows - 1, 2, modes), vmem(modes, 2, 2), vmem(rows - 1, modes), vmem(rows - 1, modes),
            ],
            in_specs=[anywhere] * 5,
            out_specs=[local] * 4,
            scratch_shapes=[
                vmem(rows, 2, modes),
                vmem(4, modes), vmem(4, modes), vmem(), vmem(parts), vmem(parts, 4), vmem(parts, 2, 2),
                vmem(rows - 1, modes),
                flat(levels), flat(levels), flat(), flat(2), vmem(modes),
                pltpu.VMEM((modes, LANES), f32), smem(rows), smem(rows), smem(kx),
                dma(5), dma(modes), dma(modes), dma(modes), dma(modes),
                dma(modes), dma(parts), dma(modes), dma(parts), dma(parts), dma(modes),
            ],
            compiler_params=pltpu.CompilerParams(collective_id=0, has_side_effects=True),
        )(
            source_field.reshape(rows, 2, modes, 2, LANES),
            coupling_below, coupling_above, eigen_stream, eigen_span.reshape(modes, LANES),
        )
        return pl.pallas_call(
            combine_kernel,
            out_shape=jax.ShapeDtypeStruct((rows, 2, kx // modes, modes * LANES), f32),
            in_specs=[local] * 4,
            out_specs=anywhere,
            scratch_shapes=[pltpu.VMEM((rows, 2, kx // modes, modes * LANES), f32), dma(rows // 8)],
            compiler_params=pltpu.CompilerParams(vmem_limit_bytes=4 << 20),
        )(*[pltpu.with_memory_space_constraint(x, pltpu.VMEM) for x in arrived])

    return jax.shard_map(
        per_device,
        mesh=mesh,
        in_specs=(P("gz", None, None, "modes"), P("gz"), P("gz"), P(), P()),
        out_specs=P("gz", None, "modes", None),
        check_vma=False,
    )
```
